32 devices in a mesh: dp: 2 (over x), tp: 16 (over y, z, core).
Axes of the slice: x: 2, y: 2, z: 4, core: 2. Of those that a mesh axis runs over, the one named last changes fastest.
Arguments:
- x: bfloat16 [4096, 7168], P('dp'), parts along dimension 0
- w_gate: bfloat16 [7168, 20480], P(None, 'tp')
- w_up: bfloat16 [7168, 20480], P(None, 'tp')
- w_down: bfloat16 [20480, 7168], P('tp')
Outputs:
- output: bfloat16 [4096, 7168], P('dp'), parts along dimension 0
There are 2 independent parts. The reference program is written for one: setup_inputs(seed, part) draws one part's arguments, and reference() takes and returns one part's arrays. A program takes and returns all parts, laid end to end along the dimension named above; an argument that names none is the same for every part.
All inputs are finite; a program needn't handle non-finite values.
Results may differ from the reference program's by a relative error of at most 0.016.
Values are sent between devices in bfloat16 or wider.
A program may use at most 2 GiB of HBM per device.

```python
import jax
import jax.numpy as jnp

ROWS = 2048
D = 7168
FF = 20480


def setup_inputs(seed: int = 0, part: int = 0) -> dict:
    kx, kg, ku, kd = jax.random.split(jax.random.key(seed), 4)
    drawn = {
        "x": jax.random.normal(jax.random.fold_in(kx, part), (ROWS, D), jnp.float32),
        "w_gate": jax.random.normal(kg, (D, FF), jnp.float32) * D**-0.5,
        "w_up": jax.random.normal(ku, (D, FF), jnp.float32) * D**-0.5,
        "w_down": jax.random.normal(kd, (FF, D), jnp.float32) * FF**-0.5,
    }
    return {k: v.astype(jnp.bfloat16) for k, v in drawn.items()}


def reference(x, w_gate, w_up, w_down):
    gate = jnp.dot(x, w_gate, preferred_element_type=jnp.float32)
    up = jnp.dot(x, w_up, preferred_element_type=jnp.float32)
    hidden = (jax.nn.silu(gate) * up).astype(jnp.bfloat16)
    return jnp.dot(hidden, w_down, preferred_element_type=jnp.float32).astype(jnp.bfloat16)
```

```python
import functools

import jax
import jax.numpy as jnp
from jax import lax
from jax.experimental import pallas as pl
from jax.experimental.pallas import tpu as pltpu
from jax.sharding import PartitionSpec as P

MESH = pl.DeviceIdType.MESH
F32, BF16 = jnp.float32, jnp.bfloat16
SLOTS = 4


def _tree(unit):
    parent = {}
    for y in range(2):
        for z in range(4):
            p = 4 * y + z
            if unit < 4:
                line = unit // 2
                root = 1 + line
                if y != line:
                    parent[p] = 4 * line + z
                else:
                    parent[p] = None if z == root else (p + 1 if z < root else p - 1)
            else:
                q = unit - 4
                if z != q:
                    parent[p] = p + 1 if z < q else p - 1
                else:
                    parent[p] = None if y == q % 2 else 4 * (1 - y) + z
    children = {p: [c for c in range(8) if parent[c] == p] for p in range(8)}

    def height(p):
        return 1 + max((height(c) for c in children[p]), default=-1)

    def depth(p):
        return 0 if parent[p] is None else 1 + depth(parent[p])

    return parent, children, [height(p) for p in range(8)], [depth(p) for p in range(8)]


TREES = [_tree(u) for u in range(8)]


def _landing(unit, p, k):
    if unit < 4:
        return 3 * (unit % 2) + k
    z, q = p % 4, unit - 4
    return k if z == q else 2 + (q - z) % 4


MAX_HEIGHT = max(max(t[2]) for t in TREES)
MAX_DEPTH = max(max(t[3]) for t in TREES)

ORDER = (
    ("X", 4), ("d", 0), ("d", 1), ("R", 0, 1), ("d", 2), ("R", 3, 2), ("d", 3), ("B", 3, 3), ("d", 4), ("R", 1, 1), ("d", 5),
    ("R", 4, 2), ("B", 1, 2), ("d", 6), ("S", 0), ("g", 0), ("B", 4, 3), ("F", 3), ("g", 1), ("R", 2, 1), ("B", 2, 2), ("g", 2),
)


def _kernel(cfg, x_hbm, wg_hbm, wu_hbm, wd_hbm, y_hbm, xb, wgb, wub, wdb, hb, own, stage, pbuf, sbuf, fbuf, ry, rz,
            xsem, gsem, usem, dsem, stsem, psem, ssem, rysem, rzsem, bsem, ysem, fssem, frsem):
    nb, rows, half_cols, yc, zc, gw, dt = (cfg[k] for k in ("nb", "rows", "half", "yc", "zc", "gw", "dt"))
    mine = rows // 2
    ng = wg_hbm.shape[1] // gw
    nt = half_cols // dt
    wslots = wdb.shape[0]
    chunks = 2 * nb

    dp = lax.axis_index("dp")
    me = lax.axis_index("tp")
    core = me % 2
    pos = me // 2
    partner = me + 1 - 2 * core

    def select(values):
        values = [0 if v is None else v for v in values]
        if all(v == values[0] for v in values):
            return values[0]
        out = jnp.int32(values[0])
        for p in range(1, 8):
            out = jnp.where(pos == p, jnp.int32(values[p]), out)
        return out

    def among(positions):
        out = pos == positions[0]
        for p in positions[1:]:
            out = jnp.logical_or(out, pos == p)
        return out

    def remote(src, dst, send, recv, device):
        return pltpu.make_async_remote_copy(
            src_ref=src, dst_ref=dst, send_sem=send, recv_sem=recv, device_id=(dp, device), device_id_type=MESH
        )

    def columns(u):
        return slice(u * yc, (u + 1) * yc) if u < 4 else slice(4 * yc + (u - 4) * zc, 4 * yc + (u - 3) * zc)

    def landed(u, slot, index):
        return (ry.at[slot, index], rysem.at[slot, index]) if u < 4 else (rz.at[slot, index], rzsem.at[slot, index])

    def load_x(b):
        slot = b % 2
        first = pl.multiple_of(b * rows + core * mine, mine)
        second = pl.multiple_of(b * rows + (1 - core) * mine, mine)
        return (
            pltpu.make_async_copy(x_hbm.at[pl.ds(first, mine)], xb.at[slot, pl.ds(0, mine)], xsem.at[slot, 0]),
            pltpu.make_async_copy(x_hbm.at[pl.ds(second, mine)], xb.at[slot, pl.ds(mine, mine)], xsem.at[slot, 1]),
        )

    def load_g(s):
        slot = s % 2
        cols = pl.ds(pl.multiple_of((s % ng) * gw, gw), gw)
        return (
            pltpu.make_async_copy(wg_hbm.at[:, cols], wgb.at[slot], gsem.at[slot]),
            pltpu.make_async_copy(wu_hbm.at[:, cols], wub.at[slot], usem.at[slot]),
        )

    def load_d(t):
        slot = t % wslots
        cols = pl.ds(pl.multiple_of((t % (2 * nt)) * dt, dt), dt)
        return (pltpu.make_async_copy(wd_hbm.at[:, cols], wdb.at[slot], dsem.at[slot]),)

    def start(copies):
        for copy in copies:
            copy.start()

    def wait(copies):
        for copy in copies:
            copy.wait()

    def gate_step(b, g):
        s = b * ng + g
        slot = s % 2
        wait(load_g(s))
        xv = xb.at[b % 2]
        gate = jnp.dot(xv[...], wgb[slot], preferred_element_type=F32)
        up = jnp.dot(xv[...], wub[slot], preferred_element_type=F32)
        hb[b % 2, :, pl.ds(pl.multiple_of(g * gw, gw), gw)] = (jax.nn.silu(gate) * up).astype(BF16)

        @pl.when(s + 2 < nb * ng)
        def _():
            start(load_g(s + 2))

    def down_step(b, half, j):
        t = b * 2 * nt + half * nt + j
        slot = (2 * b + half) % SLOTS
        wait(load_d(t))
        term = jnp.dot(hb[b % 2], wdb[t % wslots], preferred_element_type=F32)
        cols = slice(j * dt, (j + 1) * dt)
        own[slot, :, cols] = term[:mine]
        stage[slot, :, cols] = term[mine:].astype(BF16)

        @pl.when(t + wslots < nb * 2 * nt)
        def _():
            start(load_d(t + wslots))

    def to_partner(slot):
        return remote(stage.at[slot], pbuf.at[slot], stsem.at[slot], psem.at[slot], partner)

    def up_copy(u, slot):
        parent = TREES[u][0]
        place = [None if parent[p] is None else _landing(u, parent[p], TREES[u][1][parent[p]].index(p)) for p in range(8)]
        dst, sem = landed(u, slot, select(place))
        target = 2 * select([parent[p] for p in range(8)]) + core
        return remote(sbuf.at[slot, :, columns(u)], dst, ssem.at[slot, u, 0], sem, target)

    def down_copy(u, slot, k):
        children = TREES[u][1]
        target = 2 * select([children[p][k] if k < len(children[p]) else None for p in range(8)]) + core
        piece = fbuf.at[slot, :, columns(u)]
        return remote(piece, piece, ssem.at[slot, u, 1 + k], bsem.at[slot, u], target)

    def groups(u, level, kind):
        parent, children, height, depth = TREES[u]
        found = {}
        for p in range(8):
            if (height if kind == "R" else depth)[p] == level:
                found.setdefault((parent[p] is None, len(children[p])), []).append(p)
        return sorted(found.items())

    def reduce_level(slot, level):
        if level == 0:
            to_partner(slot).wait_recv()
        for u in range(8):
            for (root, count), positions in groups(u, level, "R"):

                @pl.when(among(positions))
                def _(u=u, root=root, count=count):
                    cols = columns(u)
                    total = own[slot, :, cols] + pbuf[slot, :, cols].astype(F32)
                    for k in range(count):
                        index = select([_landing(u, p, k) for p in range(8)])
                        src, sem = landed(u, slot, index)
                        remote(src, src, ssem.at[slot, u, 0], sem, me).wait_recv()
                        total = total + src[...].astype(F32)
                    out = fbuf if root else sbuf
                    out[slot, :, cols] = total.astype(BF16)
                    if root:
                        for k in range(count):
                            down_copy(u, slot, k).start()
                    else:
                        up_copy(u, slot).start()

    def broadcast_level(slot, level):
        for u in range(8):
            for (_, count), positions in groups(u, level, "B"):

                @pl.when(among(positions))
                def _(u=u, count=count):
                    down_copy(u, slot, 0).wait_recv()
                    for k in range(count):
                        down_copy(u, slot, k).start()

    def finished(c, parity):
        slot = c % SLOTS
        piece = y_hbm.at[
            pl.ds(pl.multiple_of((c // 2) * rows + core * mine, mine), mine), pl.ds(parity * half_cols, half_cols)
        ]
        return (
            pltpu.make_async_copy(fbuf.at[slot], piece, ysem.at[slot]),
            remote(fbuf.at[slot], piece, fssem.at[slot], frsem.at[slot], partner),
        )

    def settle(c, parity):
        slot = c % SLOTS
        to_partner(slot).wait_send()
        for u in range(8):
            parent, children, _, _ = TREES[u]

            @pl.when(among([p for p in range(8) if parent[p] is not None]))
            def _(u=u):
                up_copy(u, slot).wait_send()

            for k in range(3):
                have = [p for p in range(8) if len(children[p]) > k]
                if have:

                    @pl.when(among(have))
                    def _(u=u, k=k):
                        down_copy(u, slot, k).wait_send()

        local, other = finished(c, parity)
        local.wait()
        other.wait()

    start(load_x(0))
    start(load_g(0))
    start(load_g(1))
    start(load_x(1))
    for t in range(wslots):
        start(load_d(t))

    barrier = pltpu.get_barrier_semaphore()
    z = pos % 4
    rung = (me + 8) % 16

    def greet(device):
        pl.semaphore_signal(barrier, inc=1, device_id=(dp, device), device_id_type=MESH)

    greet(partner)
    greet(rung)

    @pl.when(z > 0)
    def _():
        greet(me - 2)

    @pl.when(z < 3)
    def _():
        greet(me + 2)

    pl.semaphore_wait(barrier, 3 + jnp.where(jnp.logical_or(z == 0, z == 3), 0, 1))

    wait(load_x(0))

    @pl.loop(0, ng)
    def _(g):
        gate_step(0, g)

    split = (ng + 1) // 2

    @pl.loop(0, nb + 2)
    def _(b):
        computing = b < nb
        more = b + 1 < nb

        @pl.when(b + 2 < nb)
        def _():
            start(load_x(b + 2))

        @pl.when(more)
        def _():
            wait(load_x(b + 1))

        for half in range(2):
            for item in cfg["order"]:
                kind = item[0]
                if kind == "d":
                    if item[1] < nt:

                        @pl.when(computing)
                        def _(half=half, j=item[1]):
                            down_step(b, half, j)

                elif kind == "g":
                    g = item[1] + (split if half else 0)
                    if g < (ng if half else split):

                        @pl.when(more)
                        def _(g=g):
                            gate_step(b + 1, g)

                else:
                    lag = item[-1]
                    c = 2 * b + half - lag
                    parity = (half - lag) % 2

                    @pl.when(jnp.logical_and(c >= 0, c < chunks))
                    def _(kind=kind, item=item, c=c, parity=parity):
                        slot = c % SLOTS
                        if kind == "S":
                            to_partner(slot).start()
                        elif kind == "R":
                            reduce_level(slot, item[1])
                        elif kind == "B":
                            broadcast_level(slot, item[1])
                        elif kind == "F":
                            start(finished(c, parity))
                        elif kind == "X":
                            settle(c, parity)


def build(mesh, cfg):
    def step(x, w_gate, w_up, w_down):
        d = x.shape[1]
        rows, mine = cfg["rows"], cfg["rows"] // 2
        hidden = w_gate.shape[1]
        dma = pltpu.SemaphoreType.DMA
        any_spec = pl.BlockSpec(memory_space=pl.ANY)
        return pl.pallas_call(
            functools.partial(_kernel, cfg),
            name="mlp",
            out_shape=jax.ShapeDtypeStruct(x.shape, BF16),
            in_specs=[any_spec] * 4,
            out_specs=any_spec,
            scratch_shapes=[
                pltpu.VMEM((2, rows, d), BF16),
                pltpu.VMEM((2, d, cfg["gw"]), BF16),
                pltpu.VMEM((2, d, cfg["gw"]), BF16),
                pltpu.VMEM((4, hidden, cfg["dt"]), BF16),
                pltpu.VMEM((2, rows, hidden), BF16),
                pltpu.VMEM((SLOTS, mine, cfg["half"]), F32),
                pltpu.VMEM((SLOTS, mine, cfg["half"]), BF16),
                pltpu.VMEM((SLOTS, mine, cfg["half"]), BF16),
                pltpu.VMEM((SLOTS, mine, cfg["half"]), BF16),
                pltpu.VMEM((SLOTS, mine, cfg["half"]), BF16),
                pltpu.VMEM((SLOTS, 6, mine, cfg["yc"]), BF16),
                pltpu.VMEM((SLOTS, 6, mine, cfg["zc"]), BF16),
                dma((2, 2)),
                dma((2,)),
                dma((2,)),
                dma((4,)),
                dma((SLOTS,)),
                dma((SLOTS,)),
                dma((SLOTS, 8, 4)),
                dma((SLOTS, 6)),
                dma((SLOTS, 6)),
                dma((SLOTS, 8)),
                dma((SLOTS,)),
                dma((SLOTS,)),
                dma((SLOTS,)),
            ],
            compiler_params=pltpu.CompilerParams(
                collective_id=0, has_side_effects=True, vmem_limit_bytes=67043328
            ),
        )(x, w_gate, w_up, w_down)

    return jax.shard_map(
        step,
        mesh=mesh,
        in_specs=(P("dp", None), P(None, "tp"), P(None, "tp"), P("tp", None)),
        out_specs=P("dp", None),
        check_vma=False,
    )


def solution(mesh):
    return build(mesh, dict(nb=8, rows=256, half=3584, yc=512, zc=384, gw=256, dt=512, order=ORDER))
```

```python
import functools

import jax
import jax.numpy as jnp
from jax import lax
from jax.experimental import pallas as pl
from jax.experimental.pallas import tpu as pltpu
from jax.sharding import PartitionSpec as P

MESH = pl.DeviceIdType.MESH
F32, BF16 = jnp.float32, jnp.bfloat16


def _tree(unit):
    parent = {}
    for y in range(2):
        for z in range(4):
            p = 4 * y + z
            if unit < 4:
                line = unit // 2
                root = 1 + line
                if y != line:
                    parent[p] = 4 * line + z
                else:
                    parent[p] = None if z == root else (p + 1 if z < root else p - 1)
            else:
                q = unit - 4
                if z != q:
                    parent[p] = p + 1 if z < q else p - 1
                else:
                    parent[p] = None if y == q % 2 else 4 * (1 - y) + z
    children = {p: [c for c in range(8) if parent[c] == p] for p in range(8)}

    def height(p):
        return 1 + max((height(c) for c in children[p]), default=-1)

    def depth(p):
        return 0 if parent[p] is None else 1 + depth(parent[p])

    return parent, children, [height(p) for p in range(8)], [depth(p) for p in range(8)]


TREES = [_tree(u) for u in range(8)]


def _landing(unit, p, k):
    if unit < 4:
        return 3 * (unit % 2) + k
    z, q = p % 4, unit - 4
    return k if z == q else 2 + (q - z) % 4


ORDER = (
    ("R", 0, (0, 2), 1), ("R", 3, (0, 2), 2), ("d", 0), ("R", 3, (5, 6), 2), ("F", 5), ("d", 1), ("d", 2), ("R", 0, (4, 7), 1),
    ("R", 0, (1, 3), 1), ("R", 1, (4, 7), 1), ("B", 2, (5, 6), 3), ("B", 3, (4, 7), 4), ("R", 3, (1, 3), 2),
    ("R", 0, (5, 6), 1), ("d", 3), ("B", 3, (0, 2), 4), ("B", 2, (4, 7), 3), ("g", 0), ("B", 3, (1, 3), 4),
    ("R", 3, (4, 7), 2), ("d", 4), ("R", 1, (0, 2), 1), ("B", 2, (0, 2), 3), ("d", 5), ("R", 1, (5, 6), 1),
    ("B", 2, (1, 3), 3), ("R", 4, (4, 7), 2), ("d", 6), ("B", 1, (0, 2), 2), ("S", 0), ("B", 1, (5, 6), 2), ("g", 1),
    ("R", 2, (0, 2), 1), ("R", 2, (4, 7), 1), ("R", 2, (5, 6), 1), ("R", 1, (1, 3), 1), ("B", 4, (4, 7), 4), ("g", 2),
    ("R", 2, (1, 3), 1), ("B", 1, (1, 3), 2), ("B", 3, (5, 6), 4), ("B", 1, (4, 7), 2),
)
OWN, STAGE, PBUF, SBUF, FBUF, RBUF = 3, 2, 4, 4, 6, 4
HAND = min((item[3], k) for k, item in enumerate(ORDER) if item[0] == "R")[1]


def _kernel(cfg, x_hbm, wg_hbm, wu_hbm, wd_hbm, y_hbm, xb, wgb, wub, wdb, hb, own, stage, pbuf, sbuf, fbuf, ry, rz,
            xsem, gsem, usem, dsem, stsem, psem, upsem, downsem, rysem, rzsem, bsem, ysem, fssem, frsem):
    nb, rows, half_cols, yc, zc, gw, dt = (cfg[k] for k in ("nb", "rows", "half", "yc", "zc", "gw", "dt"))
    mine = rows // 2
    ng = wg_hbm.shape[1] // gw
    nt = half_cols // dt
    wslots = wdb.shape[0]
    chunks = 2 * nb

    dp = lax.axis_index("dp")
    me = lax.axis_index("tp")
    core = me % 2
    pos = me // 2
    partner = me + 1 - 2 * core

    def select(values):
        values = [0 if v is None else v for v in values]
        if all(v == values[0] for v in values):
            return values[0]
        out = jnp.int32(values[0])
        for p in range(1, 8):
            out = jnp.where(pos == p, jnp.int32(values[p]), out)
        return out

    def among(positions):
        out = pos == positions[0]
        for p in positions[1:]:
            out = jnp.logical_or(out, pos == p)
        return out

    def remote(src, dst, send, recv, device):
        return pltpu.make_async_remote_copy(
            src_ref=src, dst_ref=dst, send_sem=send, recv_sem=recv, device_id=(dp, device), device_id_type=MESH
        )

    def columns(u):
        return slice(u * yc, (u + 1) * yc) if u < 4 else slice(4 * yc + (u - 4) * zc, 4 * yc + (u - 3) * zc)

    def landed(u, c, index):
        slot = c % RBUF
        return (ry.at[slot, index], rysem.at[slot, index]) if u < 4 else (rz.at[slot, index], rzsem.at[slot, index])

    def load_x(b):
        slot = b % 2
        first = pl.multiple_of(b * rows + core * mine, mine)
        second = pl.multiple_of(b * rows + (1 - core) * mine, mine)
        return (
            pltpu.make_async_copy(x_hbm.at[pl.ds(first, mine)], xb.at[slot, pl.ds(0, mine)], xsem.at[slot, 0]),
            pltpu.make_async_copy(x_hbm.at[pl.ds(second, mine)], xb.at[slot, pl.ds(mine, mine)], xsem.at[slot, 1]),
        )

    def load_g(s):
        slot = s % 2
        cols = pl.ds(pl.multiple_of((s % ng) * gw, gw), gw)
        return (
            pltpu.make_async_copy(wg_hbm.at[:, cols], wgb.at[slot], gsem.at[slot]),
            pltpu.make_async_copy(wu_hbm.at[:, cols], wub.at[slot], usem.at[slot]),
        )

    def load_d(t):
        slot = t % wslots
        cols = pl.ds(pl.multiple_of((t % (2 * nt)) * dt, dt), dt)
        return (pltpu.make_async_copy(wd_hbm.at[:, cols], wdb.at[slot], dsem.at[slot]),)

    def start(copies):
        for copy in copies:
            copy.start()

    def wait(copies):
        for copy in copies:
            copy.wait()

    def gate_step(b, g):
        s = b * ng + g
        slot = s % 2
        wait(load_g(s))
        xv = xb.at[b % 2]
        gate = jnp.dot(xv[...], wgb[slot], preferred_element_type=F32)
        up = jnp.dot(xv[...], wub[slot], preferred_element_type=F32)
        hb[b % 2, :, pl.ds(pl.multiple_of(g * gw, gw), gw)] = (jax.nn.silu(gate) * up).astype(BF16)

        @pl.when(s + 2 < nb * ng)
        def _():
            start(load_g(s + 2))

    def down_step(b, half, j):
        t = b * 2 * nt + half * nt + j
        c = 2 * b + half
        wait(load_d(t))
        term = jnp.dot(hb[b % 2], wdb[t % wslots], preferred_element_type=F32)
        cols = slice(j * dt, (j + 1) * dt)
        own[c % OWN, :, cols] = term[:mine]
        stage[c % STAGE, :, cols] = term[mine:].astype(BF16)

        @pl.when(t + wslots < nb * 2 * nt)
        def _():
            start(load_d(t + wslots))

    def to_partner(c):
        return remote(stage.at[c % STAGE], pbuf.at[c % PBUF], stsem.at[c % STAGE], psem.at[c % PBUF], partner)

    def up_copy(u, c):
        parent = TREES[u][0]
        place = [None if parent[p] is None else _landing(u, parent[p], TREES[u][1][parent[p]].index(p)) for p in range(8)]
        dst, sem = landed(u, c, select(place))
        target = 2 * select([parent[p] for p in range(8)]) + core
        return remote(sbuf.at[c % SBUF, :, columns(u)], dst, upsem.at[c % SBUF, u], sem, target)

    def down_copy(u, c, k):
        children = TREES[u][1]
        target = 2 * select([children[p][k] if k < len(children[p]) else None for p in range(8)]) + core
        piece = fbuf.at[c % FBUF, :, columns(u)]
        return remote(piece, piece, downsem.at[c % FBUF, u, k], bsem.at[c % FBUF, u], target)

    def groups(u, level, kind):
        parent, children, height, depth = TREES[u]
        found = {}
        for p in range(8):
            if (height if kind == "R" else depth)[p] == level:
                found.setdefault((parent[p] is None, len(children[p])), []).append(p)
        return sorted(found.items())

    def reduce_level(c, level, units):
        for u in units:
            for (root, count), positions in groups(u, level, "R"):

                @pl.when(among(positions))
                def _(u=u, root=root, count=count):
                    cols = columns(u)
                    total = own[c % OWN, :, cols] + pbuf[c % PBUF, :, cols].astype(F32)
                    for k in range(count):
                        src, sem = landed(u, c, select([_landing(u, p, k) for p in range(8)]))
                        remote(src, src, upsem.at[c % SBUF, u], sem, me).wait_recv()
                        total = total + src[...].astype(F32)
                    if root:
                        fbuf[c % FBUF, :, cols] = total.astype(BF16)
                        for k in range(count):
                            down_copy(u, c, k).start()
                    else:
                        sbuf[c % SBUF, :, cols] = total.astype(BF16)
                        up_copy(u, c).start()

    def broadcast_level(c, level, units):
        for u in units:
            for (_, count), positions in groups(u, level, "B"):

                @pl.when(among(positions))
                def _(u=u, count=count):
                    down_copy(u, c, 0).wait_recv()
                    for k in range(count):
                        down_copy(u, c, k).start()

    def finished(c, parity):
        slot = c % FBUF
        piece = y_hbm.at[
            pl.ds(pl.multiple_of((c // 2) * rows + core * mine, mine), mine), pl.ds(parity * half_cols, half_cols)
        ]
        return (
            pltpu.make_async_copy(fbuf.at[slot], piece, ysem.at[slot]),
            remote(fbuf.at[slot], piece, fssem.at[slot], frsem.at[slot], partner),
        )

    def settle_up(c):
        for u in range(8):
            parent = TREES[u][0]

            @pl.when(among([p for p in range(8) if parent[p] is not None]))
            def _(u=u):
                up_copy(u, c).wait_send()

    def settle_down(c, parity):
        for u in range(8):
            for k in range(3):
                have = [p for p in range(8) if len(TREES[u][1][p]) > k]
                if have:

                    @pl.when(among(have))
                    def _(u=u, k=k):
                        down_copy(u, c, k).wait_send()

        local, other = finished(c, parity)
        local.wait()
        other.wait()

    start(load_x(0))
    start(load_g(0))
    start(load_g(1))
    start(load_x(1))
    for t in range(wslots):
        start(load_d(t))

    barrier = pltpu.get_barrier_semaphore()
    z = pos % 4
    rung = (me + 8) % 16

    def greet(device):
        pl.semaphore_signal(barrier, inc=1, device_id=(dp, device), device_id_type=MESH)

    greet(partner)
    greet(rung)

    @pl.when(z > 0)
    def _():
        greet(me - 2)

    @pl.when(z < 3)
    def _():
        greet(me + 2)

    pl.semaphore_wait(barrier, 3 + jnp.where(jnp.logical_or(z == 0, z == 3), 0, 1))

    wait(load_x(0))

    @pl.loop(0, ng)
    def _(g):
        gate_step(0, g)

    split = (ng + 1) // 2

    @pl.loop(0, nb + FBUF // 2)
    def _(b):
        computing = b < nb
        more = b + 1 < nb

        @pl.when(b + 2 < nb)
        def _():
            start(load_x(b + 2))

        @pl.when(more)
        def _():
            wait(load_x(b + 1))

        for half in range(2):

            def after(lag, act, *args, half=half):
                c = 2 * b + half - lag

                @pl.when(jnp.logical_and(c >= 0, c < chunks))
                def _():
                    act(c, *args)

            after(STAGE, lambda c: to_partner(c).wait_send())
            after(SBUF, settle_up)
            after(FBUF, settle_down, (half - FBUF) % 2)
            for k, item in enumerate(cfg["order"]):
                kind = item[0]
                if k == HAND:
                    after(item[3], lambda c: to_partner(c).wait_recv())
                if kind == "d":
                    if item[1] < nt:

                        @pl.when(computing)
                        def _(half=half, j=item[1]):
                            down_step(b, half, j)

                elif kind == "g":
                    g = item[1] + (split if half else 0)
                    if g < (ng if half else split):

                        @pl.when(more)
                        def _(g=g):
                            gate_step(b + 1, g)

                elif kind == "S":
                    after(0, lambda c: to_partner(c).start())
                elif kind == "R":
                    after(item[3], reduce_level, item[1], item[2])
                elif kind == "B":
                    after(item[3], broadcast_level, item[1], item[2])
                elif kind == "F":
                    after(item[1], lambda c, parity: [p.start() for p in finished(c, parity)], (half - item[1]) % 2)


def build(mesh, cfg):
    def step(x, w_gate, w_up, w_down):
        d = x.shape[1]
        rows, mine = cfg["rows"], cfg["rows"] // 2
        hidden = w_gate.shape[1]
        dma = pltpu.SemaphoreType.DMA
        any_spec = pl.BlockSpec(memory_space=pl.ANY)
        return pl.pallas_call(
            functools.partial(_kernel, cfg),
            name="mlp",
            out_shape=jax.ShapeDtypeStruct(x.shape, BF16),
            in_specs=[any_spec] * 4,
            out_specs=any_spec,
            scratch_shapes=[
                pltpu.VMEM((2, rows, d), BF16),
                pltpu.VMEM((2, d, cfg["gw"]), BF16),
                pltpu.VMEM((2, d, cfg["gw"]), BF16),
                pltpu.VMEM((4, hidden, cfg["dt"]), BF16),
                pltpu.VMEM((2, rows, hidden), BF16),
                pltpu.VMEM((OWN, mine, cfg["half"]), F32),
                pltpu.VMEM((STAGE, mine, cfg["half"]), BF16),
                pltpu.VMEM((PBUF, mine, cfg["half"]), BF16),
                pltpu.VMEM((SBUF, mine, cfg["half"]), BF16),
                pltpu.VMEM((FBUF, mine, cfg["half"]), BF16),
                pltpu.VMEM((RBUF, 6, mine, cfg["yc"]), BF16),
                pltpu.VMEM((RBUF, 6, mine, cfg["zc"]), BF16),
                dma((2, 2)),
                dma((2,)),
                dma((2,)),
                dma((4,)),
                dma((STAGE,)),
                dma((PBUF,)),
                dma((SBUF, 8)),
                dma((FBUF, 8, 3)),
                dma((RBUF, 6)),
                dma((RBUF, 6)),
                dma((FBUF, 8)),
                dma((FBUF,)),
                dma((FBUF,)),
                dma((FBUF,)),
            ],
            compiler_params=pltpu.CompilerParams(
                collective_id=0, has_side_effects=True, vmem_limit_bytes=67043328
            ),
        )(x, w_gate, w_up, w_down)

    return jax.shard_map(
        step,
        mesh=mesh,
        in_specs=(P("dp", None), P(None, "tp"), P(None, "tp"), P("tp", None)),
        out_specs=P("dp", None),
        check_vma=False,
    )


def solution(mesh):
    return build(mesh, dict(nb=8, rows=256, half=3584, yc=512, zc=384, gw=256, dt=512, order=ORDER))
```

```python
import functools

import jax
import jax.numpy as jnp
from jax import lax
from jax.experimental import pallas as pl
from jax.experimental.pallas import tpu as pltpu
from jax.sharding import PartitionSpec as P

MESH = pl.DeviceIdType.MESH
F32, BF16 = jnp.float32, jnp.bfloat16


def _tree(unit):
    parent = {}
    for y in range(2):
        for z in range(4):
            p = 4 * y + z
            if unit < 4:
                line = unit // 2
                root = 1 + line
                if y != line:
                    parent[p] = 4 * line + z
                else:
                    parent[p] = None if z == root else (p + 1 if z < root else p - 1)
            else:
                q = unit - 4
                if z != q:
                    parent[p] = p + 1 if z < q else p - 1
                else:
                    parent[p] = None if y == q % 2 else 4 * (1 - y) + z
    children = {p: [c for c in range(8) if parent[c] == p] for p in range(8)}

    def height(p):
        return 1 + max((height(c) for c in children[p]), default=-1)

    def depth(p):
        return 0 if parent[p] is None else 1 + depth(parent[p])

    return parent, children, [height(p) for p in range(8)], [depth(p) for p in range(8)]


TREES = [_tree(u) for u in range(8)]


def _landing(unit, p, k):
    if unit < 4:
        return 3 * (unit % 2) + k
    z, q = p % 4, unit - 4
    return k if z == q else 2 + (q - z) % 4


ORDER = (
    ("d", 0), ("F", 5), ("R", 0, (1, 3), 1), ("B", 3, (0, 2), 4), ("B", 1, (1, 3), 3), ("d", 1), ("R", 3, (5, 6), 2),
    ("d", 2), ("d", 3), ("R", 3, (4, 7), 2), ("B", 2, (1, 3), 4), ("R", 1, (4, 7), 1), ("R", 3, (0, 2), 2), ("g", 0),
    ("B", 3, (4, 7), 4), ("R", 1, (0, 2), 1), ("d", 4), ("R", 1, (5, 6), 1), ("d", 5), ("B", 2, (4, 7), 3), ("d", 6),
    ("R", 4, (4, 7), 2), ("R", 3, (1, 3), 2), ("S", 0), ("R", 1, (1, 3), 1), ("R", 2, (4, 7), 1), ("g", 1),
    ("R", 2, (5, 6), 1), ("B", 1, (0, 2), 2), ("B", 2, (0, 2), 3), ("R", 2, (0, 2), 1), ("g", 2), ("B", 1, (5, 6), 2),
    ("B", 2, (5, 6), 3), ("R", 0, (0, 2), 0), ("R", 0, (4, 7), 0), ("B", 4, (4, 7), 4), ("B", 1, (4, 7), 2),
    ("R", 2, (1, 3), 1), ("B", 3, (5, 6), 4), ("B", 3, (1, 3), 4), ("R", 0, (5, 6), 0),
)
OWN, STAGE, PBUF, SBUF, FBUF, RBUF = 3, 2, 4, 4, 6, 4
HAND = min((item[3], k) for k, item in enumerate(ORDER) if item[0] == "R")[1]


def _kernel(cfg, x_hbm, wg_hbm, wu_hbm, wd_hbm, y_hbm, xb, wgb, wub, wdb, hb, own, stage, pbuf, sbuf, fbuf, ry, rz,
            xsem, gsem, usem, dsem, stsem, psem, upsem, downsem, rysem, rzsem, bsem, ysem, fssem, frsem):
    nb, rows, half_cols, yc, zc, gw, dt = (cfg[k] for k in ("nb", "rows", "half", "yc", "zc", "gw", "dt"))
    mine = rows // 2
    ng = wg_hbm.shape[1] // gw
    nt = half_cols // dt
    gslots, wslots = wgb.shape[0], wdb.shape[0]
    chunks = 2 * nb

    dp = lax.axis_index("dp")
    me = lax.axis_index("tp")
    core = me % 2
    pos = me // 2 + core * (7 - 2 * (me // 2))
    partner = me + 1 - 2 * core

    def select(values):
        values = [0 if v is None else v for v in values]
        if all(v == values[0] for v in values):
            return values[0]
        out = jnp.int32(values[0])
        for p in range(1, 8):
            out = jnp.where(pos == p, jnp.int32(values[p]), out)
        return out

    def among(positions):
        out = pos == positions[0]
        for p in positions[1:]:
            out = jnp.logical_or(out, pos == p)
        return out

    def device(position):
        return 2 * (position + core * (7 - 2 * position)) + core

    def remote(src, dst, send, recv, target):
        return pltpu.make_async_remote_copy(
            src_ref=src, dst_ref=dst, send_sem=send, recv_sem=recv, device_id=(dp, target), device_id_type=MESH
        )

    def columns(u):
        return slice(u * yc, (u + 1) * yc) if u < 4 else slice(4 * yc + (u - 4) * zc, 4 * yc + (u - 3) * zc)

    def landed(u, c, index):
        slot = c % RBUF
        return (ry.at[slot, index], rysem.at[slot, index]) if u < 4 else (rz.at[slot, index], rzsem.at[slot, index])

    def load_x(b):
        slot = b % 2
        first = pl.multiple_of(b * rows + core * mine, mine)
        second = pl.multiple_of(b * rows + (1 - core) * mine, mine)
        return (
            pltpu.make_async_copy(x_hbm.at[pl.ds(first, mine)], xb.at[slot, pl.ds(0, mine)], xsem.at[slot, 0]),
            pltpu.make_async_copy(x_hbm.at[pl.ds(second, mine)], xb.at[slot, pl.ds(mine, mine)], xsem.at[slot, 1]),
        )

    def load_g(s):
        slot = s % gslots
        cols = pl.ds(pl.multiple_of((s % ng) * gw, gw), gw)
        return (
            pltpu.make_async_copy(wg_hbm.at[:, cols], wgb.at[slot], gsem.at[slot]),
            pltpu.make_async_copy(wu_hbm.at[:, cols], wub.at[slot], usem.at[slot]),
        )

    def load_d(t):
        slot = t % wslots
        cols = pl.ds(pl.multiple_of((t % (2 * nt)) * dt, dt), dt)
        return (pltpu.make_async_copy(wd_hbm.at[:, cols], wdb.at[slot], dsem.at[slot]),)

    def start(copies):
        for copy in copies:
            copy.start()

    def wait(copies):
        for copy in copies:
            copy.wait()

    def gate_step(b, g):
        s = b * ng + g
        slot = s % gslots
        wait(load_g(s))
        xv = xb.at[b % 2]
        gate = jnp.dot(xv[...], wgb[slot], preferred_element_type=F32)
        up = jnp.dot(xv[...], wub[slot], preferred_element_type=F32)
        hb[b % 2, :, pl.ds(pl.multiple_of(g * gw, gw), gw)] = (jax.nn.silu(gate) * up).astype(BF16)

        @pl.when(s + gslots < nb * ng)
        def _():
            start(load_g(s + gslots))

    def down_step(b, half, j):
        t = b * 2 * nt + half * nt + j
        c = 2 * b + half
        wait(load_d(t))
        term = jnp.dot(hb[b % 2], wdb[t % wslots], preferred_element_type=F32)
        cols = slice(j * dt, (j + 1) * dt)
        own[c % OWN, :, cols] = term[:mine]
        stage[c % STAGE, :, cols] = term[mine:].astype(BF16)

        @pl.when(t + wslots < nb * 2 * nt)
        def _():
            start(load_d(t + wslots))

    def to_partner(c):
        return remote(stage.at[c % STAGE], pbuf.at[c % PBUF], stsem.at[c % STAGE], psem.at[c % PBUF], partner)

    def up_copy(u, c):
        parent = TREES[u][0]
        place = [None if parent[p] is None else _landing(u, parent[p], TREES[u][1][parent[p]].index(p)) for p in range(8)]
        dst, sem = landed(u, c, select(place))
        target = device(select([parent[p] for p in range(8)]))
        return remote(sbuf.at[c % SBUF, :, columns(u)], dst, upsem.at[c % SBUF, u], sem, target)

    def down_copy(u, c, k):
        children = TREES[u][1]
        target = device(select([children[p][k] if k < len(children[p]) else None for p in range(8)]))
        piece = fbuf.at[c % FBUF, :, columns(u)]
        return remote(piece, piece, downsem.at[c % FBUF, u, k], bsem.at[c % FBUF, u], target)

    def groups(u, level, kind):
        parent, children, height, depth = TREES[u]
        found = {}
        for p in range(8):
            if (height if kind == "R" else depth)[p] == level:
                found.setdefault((parent[p] is None, len(children[p])), []).append(p)
        return sorted(found.items())

    def reduce_level(c, level, units):
        for u in units:
            for (root, count), positions in groups(u, level, "R"):

                @pl.when(among(positions))
                def _(u=u, root=root, count=count):
                    cols = columns(u)
                    total = own[c % OWN, :, cols] + pbuf[c % PBUF, :, cols].astype(F32)
                    for k in range(count):
                        src, sem = landed(u, c, select([_landing(u, p, k) for p in range(8)]))
                        remote(src, src, upsem.at[c % SBUF, u], sem, me).wait_recv()
                        total = total + src[...].astype(F32)
                    if root:
                        fbuf[c % FBUF, :, cols] = total.astype(BF16)
                        for k in range(count):
                            down_copy(u, c, k).start()
                    else:
                        sbuf[c % SBUF, :, cols] = total.astype(BF16)
                        up_copy(u, c).start()

    def broadcast_level(c, level, units):
        for u in units:
            for (_, count), positions in groups(u, level, "B"):

                @pl.when(among(positions))
                def _(u=u, count=count):
                    down_copy(u, c, 0).wait_recv()
                    for k in range(count):
                        down_copy(u, c, k).start()

    def finished(c, parity):
        slot = c % FBUF
        piece = y_hbm.at[
            pl.ds(pl.multiple_of((c // 2) * rows + core * mine, mine), mine), pl.ds(parity * half_cols, half_cols)
        ]
        return (
            pltpu.make_async_copy(fbuf.at[slot], piece, ysem.at[slot]),
            remote(fbuf.at[slot], piece, fssem.at[slot], frsem.at[slot], partner),
        )

    def settle_up(c):
        for u in range(8):
            parent = TREES[u][0]

            @pl.when(among([p for p in range(8) if parent[p] is not None]))
            def _(u=u):
                up_copy(u, c).wait_send()

    def settle_down(c, parity):
        for u in range(8):
            for k in range(3):
                have = [p for p in range(8) if len(TREES[u][1][p]) > k]
                if have:

                    @pl.when(among(have))
                    def _(u=u, k=k):
                        down_copy(u, c, k).wait_send()

        local, other = finished(c, parity)
        local.wait()
        other.wait()

    start(load_x(0))
    for s in range(gslots):
        start(load_g(s))

    barrier = pltpu.get_barrier_semaphore()
    z = (me // 2) % 4
    rung = (me + 8) % 16

    def greet(target):
        pl.semaphore_signal(barrier, inc=1, device_id=(dp, target), device_id_type=MESH)

    greet(partner)
    greet(rung)

    @pl.when(z > 0)
    def _():
        greet(me - 2)

    @pl.when(z < 3)
    def _():
        greet(me + 2)

    pl.semaphore_wait(barrier, 3 + jnp.where(jnp.logical_or(z == 0, z == 3), 0, 1))

    wait(load_x(0))

    @pl.loop(0, ng)
    def _(g):
        gate_step(0, g)

        @pl.when(g == ng - gslots - 1)
        def _():
            for t in range(wslots):
                start(load_d(t))

        @pl.when(g == ng - gslots)
        def _():
            start(load_x(1))

    split = (ng + 1) // 2

    @pl.loop(0, nb + FBUF // 2)
    def _(b):
        computing = b < nb
        more = b + 1 < nb

        @pl.when(b + 2 < nb)
        def _():
            start(load_x(b + 2))

        for half in range(2):

            def after(lag, act, *args, half=half):
                c = 2 * b + half - lag

                @pl.when(jnp.logical_and(c >= 0, c < chunks))
                def _():
                    act(c, *args)

            after(STAGE, lambda c: to_partner(c).wait_send())
            after(SBUF, settle_up)
            after(FBUF, settle_down, (half - FBUF) % 2)
            for k, item in enumerate(cfg["order"]):
                kind = item[0]
                if k == HAND:
                    after(item[3], lambda c: to_partner(c).wait_recv())
                if kind == "d":
                    if item[1] < nt:

                        @pl.when(computing)
                        def _(half=half, j=item[1]):
                            down_step(b, half, j)

                elif kind == "g":
                    g = item[1] + (split if half else 0)
                    if g < (ng if half else split):

                        @pl.when(more)
                        def _(g=g):
                            if g == 0:
                                wait(load_x(b + 1))
                            gate_step(b + 1, g)

                elif kind == "S":
                    after(0, lambda c: to_partner(c).start())
                elif kind == "R":
                    after(item[3], reduce_level, item[1], item[2])
                elif kind == "B":
                    after(item[3], broadcast_level, item[1], item[2])
                elif kind == "F":
                    after(item[1], lambda c, parity: [p.start() for p in finished(c, parity)], (half - item[1]) % 2)


def build(mesh, cfg):
    def step(x, w_gate, w_up, w_down):
        d = x.shape[1]
        rows, mine = cfg["rows"], cfg["rows"] // 2
        hidden = w_gate.shape[1]
        dma = pltpu.SemaphoreType.DMA
        any_spec = pl.BlockSpec(memory_space=pl.ANY)
        return pl.pallas_call(
            functools.partial(_kernel, cfg),
            name="mlp",
            out_shape=jax.ShapeDtypeStruct(x.shape, BF16),
            in_specs=[any_spec] * 4,
            out_specs=any_spec,
            scratch_shapes=[
                pltpu.VMEM((2, rows, d), BF16),
                pltpu.VMEM((3, d, cfg["gw"]), BF16),
                pltpu.VMEM((3, d, cfg["gw"]), BF16),
                pltpu.VMEM((4, hidden, cfg["dt"]), BF16),
                pltpu.VMEM((2, rows, hidden), BF16),
                pltpu.VMEM((OWN, mine, cfg["half"]), F32),
                pltpu.VMEM((STAGE, mine, cfg["half"]), BF16),
                pltpu.VMEM((PBUF, mine, cfg["half"]), BF16),
                pltpu.VMEM((SBUF, mine, cfg["half"]), BF16),
                pltpu.VMEM((FBUF, mine, cfg["half"]), BF16),
                pltpu.VMEM((RBUF, 6, mine, cfg["yc"]), BF16),
                pltpu.VMEM((RBUF, 6, mine, cfg["zc"]), BF16),
                dma((2, 2)),
                dma((3,)),
                dma((3,)),
                dma((4,)),
                dma((STAGE,)),
                dma((PBUF,)),
                dma((SBUF, 8)),
                dma((FBUF, 8, 3)),
                dma((RBUF, 6)),
                dma((RBUF, 6)),
                dma((FBUF, 8)),
                dma((FBUF,)),
                dma((FBUF,)),
                dma((FBUF,)),
            ],
            compiler_params=pltpu.CompilerParams(
                collective_id=0, has_side_effects=True, vmem_limit_bytes=67043328
            ),
        )(x, w_gate, w_up, w_down)

    return jax.shard_map(
        step,
        mesh=mesh,
        in_specs=(P("dp", None), P(None, "tp"), P(None, "tp"), P("tp", None)),
        out_specs=P("dp", None),
        check_vma=False,
    )


def solution(mesh):
    return build(mesh, dict(nb=8, rows=256, half=3584, yc=512, zc=384, gw=256, dt=512, order=ORDER))
```
